32 devices in a mesh: groups: 2 (over x), tile: 16 (over z, y, core).
Axes of the slice: x: 2, y: 2, z: 4, core: 2. Of those that a mesh axis runs over, the one named last changes fastest.
Arguments:
- tracer: float32 [32, 6, 8, 128, 128], P(('groups', 'tile')), parts along dimension 0, may hold values from -6 to 6
- courant_east: bfloat16 [32, 6, 8, 128, 128], P(('groups', 'tile')), parts along dimension 0, may hold values from -1.5 to 1.5
- courant_north: bfloat16 [32, 6, 8, 128, 128], P(('groups', 'tile')), parts along dimension 0, may hold values from -1.5 to 1.5
- diffusivity: bfloat16 [32, 6, 8, 128, 128], P(('groups', 'tile')), parts along dimension 0, may hold values from 0.049804688 to 5
- seam_table: int32 [6, 4, 3], replicated, may hold values from 0 to 5, as said below
Outputs:
- updated: float32 [32, 6, 8, 128, 128], P(('groups', 'tile')), parts along dimension 0
The draws below stay inside these ranges and needn't reach their ends.
There are 2 independent parts, one for each index of `groups`. The reference program is written for one: setup_inputs(seed, part) draws one part's arguments, and reference() takes and returns one part's arrays. A program takes and returns all parts, laid end to end along the dimension named above; an argument that names none is the same for every part. Nothing has to cross between parts.
Inputs may be any that keep to these rules, and one draw needn't show every extreme that they name: seam_table[p, e] = (q, f, r) names the edge f of panel q != p that borders edge e of panel p, and r is 1 where their edge indices run in opposite directions, 0 otherwise; the 24 edges form 12 pairs whose entries name each other with the same r, as on the faces of a cube ; edge 3 of panel 0 borders edge 3 of panel 1.
All inputs are finite; a program needn't handle non-finite values.
Results may differ from the reference program's by a relative error of at most 0.0003.
Values sent between devices are 32-bit elements; how exact they have to be, the bound alone decides.
A program may use at most 128 MiB of HBM per device.

```python
import math
import jax
import jax.numpy as jnp
from jax import lax

CT = 128
LEVELS = 8
PANELS = 6
DEPTH = 2
SIDE = 4
N_TILE = 16


def turn_axes(first_old, second_old, quarter):
    first_axis = jnp.where(quarter == 0, first_old, jnp.where(quarter == 1, second_old, jnp.where(quarter == 2, -first_old, -second_old)))
    second_axis = jnp.where(quarter == 0, second_old, jnp.where(quarter == 1, -first_old, jnp.where(quarter == 2, -second_old, first_old)))
    return (first_axis, second_axis)


def draw_seam_table(key, part):
    normals = jnp.array([[1, 0, 0], [0, 1, 0], [0, 0, 1], [-1, 0, 0], [0, -1, 0], [0, 0, -1]], jnp.int32)
    firsts = jnp.array([[0, 1, 0], [0, 0, 1], [1, 0, 0], [0, 0, 1], [1, 0, 0], [0, 1, 0]], jnp.int32)
    seconds = jnp.array([[0, 0, 1], [1, 0, 0], [0, 1, 0], [0, 1, 0], [0, 0, 1], [1, 0, 0]], jnp.int32)
    split_keys = jax.random.split(jax.random.fold_in(key, 11), 3)
    head_label = jax.random.randint(split_keys[0], (1,), 0, 6)
    quarter = jax.random.randint(split_keys[1], (6, 1), 0, 4)
    centre_zero = normals[head_label]
    first_zero, second_zero = turn_axes(firsts[head_label], seconds[head_label], quarter[0:1])
    centre_one = -first_zero
    first_one = -centre_zero
    second_one = -second_zero
    remaining = jnp.concatenate([-centre_zero, first_zero, second_zero, -second_zero], axis=0)
    remaining = remaining[jax.random.permutation(split_keys[2], 4)]
    same_face = jnp.all(remaining[:, None, :] == normals[None, :, :], axis=-1).astype(jnp.int32)
    rest_labels = jnp.sum(same_face * jnp.arange(6, dtype=jnp.int32)[None, :], axis=1)
    first_rest, second_rest = turn_axes(firsts[rest_labels], seconds[rest_labels], quarter[2:])
    centre = jnp.concatenate([centre_zero, centre_one, remaining], axis=0)
    first_axis = jnp.concatenate([first_zero, first_one, first_rest], axis=0)
    second_axis = jnp.concatenate([second_zero, second_one, second_rest], axis=0)
    middle = jnp.stack([centre - second_axis, centre + first_axis, centre + second_axis, centre - first_axis], axis=1).reshape(24, 3)
    heading = jnp.stack([first_axis, second_axis, first_axis, second_axis], axis=1).reshape(24, 3)
    panel_of = jnp.arange(24, dtype=jnp.int32) // 4
    matches = jnp.all(middle[:, None, :] == middle[None, :, :], axis=-1) & (panel_of[:, None] != panel_of[None, :])
    partner = jnp.sum(matches.astype(jnp.int32) * jnp.arange(24, dtype=jnp.int32)[None, :], axis=1)
    partner_heading = jnp.sum(matches.astype(jnp.int32)[:, :, None] * heading[None, :, :], axis=1)
    reversal = (jnp.sum(heading * partner_heading, axis=-1) < 0).astype(jnp.int32)
    return jnp.stack([partner // 4, partner % 4, reversal], axis=-1).reshape(6, 4, 3).astype(jnp.int32)


def steps_of(key, extent, pieces, least, top_value):
    factor_of = 1.0
    for position, blocks in pieces:
        heights = jax.random.uniform(jax.random.fold_in(jax.random.fold_in(key, 6), position), (blocks,), jnp.float32, least / len(pieces), top_value / len(pieces))
        factor_of = factor_of * jnp.repeat(jnp.exp(heights), extent[position] // blocks).reshape((-1,) + (1,) * (len(extent) - 1 - position))
    return factor_of


def bell_draw(own_key, shape, width, limit, cuts=(), held_as=jnp.bfloat16):
    result = jax.random.normal(own_key, shape, jnp.float32) * width
    if len(cuts) > 0:
        result = steps_of(own_key, shape, cuts, -0.22, 0.18) * result
    return jnp.clip(result, min=-limit, max=limit).astype(held_as)


def setup_inputs(seed: int = 0, part: int = 0) -> dict:
    arg_keys = jax.random.split(jax.random.key(seed), 6)
    own_keys = jax.random.split(jax.random.fold_in(arg_keys[5], part), 6)
    tracer = bell_draw(own_keys[0], (N_TILE, PANELS, LEVELS, CT, CT), 1.0, 6.0, ((0, 16),), jnp.float32)
    courant_east = bell_draw(own_keys[1], (N_TILE, PANELS, LEVELS, CT, CT), 0.3, 1.5, ((0, 16),))
    courant_north = bell_draw(own_keys[2], (N_TILE, PANELS, LEVELS, CT, CT), 0.3, 1.5, ((0, 16),))
    diffusivity = jnp.clip(jnp.exp(math.log(5.0) - 4.609084 * jax.random.uniform(own_keys[3], (N_TILE, PANELS, LEVELS, CT, CT), jnp.float32) ** steps_of(own_keys[3], (N_TILE, PANELS, LEVELS, CT, CT), ((0, 16),), -0.2, 0.2)), 0.049804688, 5.0).astype(jnp.bfloat16)
    seam_table = draw_seam_table(jax.random.fold_in(arg_keys[5], 71), part)
    return dict(tracer=tracer, courant_east=courant_east, courant_north=courant_north, diffusivity=diffusivity, seam_table=seam_table)


def edge_strips(panels, rows_deep):
    south_rows = jnp.moveaxis(panels[:, :, :, :rows_deep], 3, 1)
    east_rows = jnp.moveaxis(panels[:, :, ::-1, :][:, :, :rows_deep, :], 2, 1)
    north_rows = jnp.moveaxis(panels[:, :, :, ::-1][:, :, :, :rows_deep], 3, 1)
    west_rows = jnp.moveaxis(panels[:, :, :rows_deep, :], 2, 1)
    return jnp.stack([south_rows, east_rows, north_rows, west_rows], axis=1)


def centered(extended, along):
    kept = extended.shape[along] - 4

    def shifted(offset):
        return lax.slice_in_dim(extended, 2 + offset, 2 + offset + kept, axis=along)

    return (8.0 * (shifted(1) - shifted(-1)) - (shifted(2) - shifted(-2))) / 12.0


def advance(panels, ghosts, courant_east, courant_north, diffusivity):
    west_part = jnp.moveaxis(ghosts[:, 3, ::-1], 1, 2)
    east_part = jnp.moveaxis(ghosts[:, 1], 1, 2)
    south_part = jnp.transpose(ghosts[:, 0, ::-1], (0, 2, 3, 1))
    north_part = jnp.transpose(ghosts[:, 2], (0, 2, 3, 1))
    along_first = jnp.concatenate([west_part, panels, east_part], axis=2)
    along_second = jnp.concatenate([south_part, panels, north_part], axis=3)
    forced = panels - (courant_east.astype(jnp.float32) * centered(along_first, 2)
                       + courant_north.astype(jnp.float32) * centered(along_second, 3))
    coupling = diffusivity.astype(jnp.float32)
    ratios = []
    partial_values = []
    for height in range(panels.shape[1]):
        diagonal = 1.0 + coupling[:, height]
        if height > 0:
            below = coupling[:, height - 1]
            pivot_value = diagonal + below - below * ratios[-1]
            current = (forced[:, height] + below * partial_values[-1]) / pivot_value
        else:
            pivot_value = diagonal
            current = forced[:, height] / pivot_value
        ratios.append(coupling[:, height] / pivot_value)
        partial_values.append(current)
    solved = [partial_values[-1]]
    for height in range(panels.shape[1] - 2, -1, -1):
        solved.insert(0, partial_values[height] + ratios[height] * solved[0])
    return jnp.stack(solved, axis=1)


def panel_offset(panel_no):
    return (panel_no % 2) * (SIDE * SIDE // 2 + 1)


def to_panels(tiles):
    aligned = jnp.stack([jnp.roll(tiles[:, panel_no], -panel_offset(panel_no), axis=0)
                         for panel_no in range(PANELS)], axis=1)
    shaped = aligned.reshape(SIDE, SIDE, PANELS, LEVELS, CT, CT)
    shaped = jnp.transpose(shaped, (2, 3, 0, 4, 1, 5))
    return shaped.reshape(PANELS, LEVELS, SIDE * CT, SIDE * CT)


def to_tiles(panels):
    shaped = panels.reshape(PANELS, LEVELS, SIDE, CT, SIDE, CT)
    shaped = jnp.transpose(shaped, (2, 4, 0, 1, 3, 5))
    aligned = shaped.reshape(SIDE * SIDE, PANELS, LEVELS, CT, CT)
    return jnp.stack([jnp.roll(aligned[:, panel_no], panel_offset(panel_no), axis=0)
                      for panel_no in range(PANELS)], axis=1)


def reference(tracer, courant_east, courant_north, diffusivity, seam_table):
    panels = to_panels(tracer)
    strips = edge_strips(panels, DEPTH)
    flat_strips = strips.reshape((PANELS * 4,) + strips.shape[2:])
    source_block = (seam_table[:, :, 0] * 4 + seam_table[:, :, 1]).reshape(-1).astype(jnp.int32)
    reverse_it = (seam_table[:, :, 2] == 1).reshape(-1)
    picked = jnp.take(flat_strips, source_block, axis=0)
    picked = jnp.where(reverse_it[:, None, None, None], picked[..., ::-1], picked)
    ghosts = picked.reshape(strips.shape)
    updated = advance(panels, ghosts, to_panels(courant_east), to_panels(courant_north), to_panels(diffusivity))
    return to_tiles(updated)
```

```python
import functools
import math

import jax
import jax.numpy as jnp
from jax import lax
from jax.experimental import pallas as pl
from jax.experimental.pallas import tpu as pltpu
from jax.sharding import PartitionSpec as P

DEPTH = 2


def tile_of(device, parity, total):
    return lax.rem(device + total - parity * (total // 2 + 1) + total, total)


def edge_state(device, parity, total, across):
    tile = tile_of(device, parity, total)
    row, col = tile // across, lax.rem(tile, across)
    on = (col == 0, row == across - 1, col == across - 1, row == 0)
    return on, (row, col, row, col)


def edge_tile(edge, spot, across):
    return (spot * across, (across - 1) * across + spot, spot * across + across - 1, spot)[edge]


def exchange_kernel(total, across, table, tracer, h_out, s_out, q, s, r, d, h,
                    q_sem, send1, r_sem, send2, h_sem, out_sem):
    panels, levels, ct, _ = q.shape
    half = panels // 2
    pieces = DEPTH * levels
    me = lax.axis_index("tile")
    steps = (total - 1, across, 1, total - across)

    for p in range(panels):
        pltpu.make_async_copy(tracer.at[p], q.at[p], q_sem.at[p]).start()

    barrier = pltpu.get_barrier_semaphore()

    def greet(i, carry):
        pl.semaphore_signal(barrier, inc=1, device_id={"tile": lax.rem(me + i, total)},
                            device_id_type=pl.DeviceIdType.MESH)
        return carry

    lax.fori_loop(1, total, greet, 0)

    def remote(src, dst, send, recv, device):
        return pltpu.make_async_remote_copy(
            src_ref=src, dst_ref=dst, send_sem=send, recv_sem=recv,
            device_id={"tile": device}, device_id_type=pl.DeviceIdType.MESH)

    lane_group = lax.broadcasted_iota(jnp.int32, (ct, 128), 1) // 4
    for parity in range(2):
        gathered = jnp.zeros((ct, 128), jnp.float32)
        for n in range(half):
            p = 2 * n + parity
            pltpu.make_async_copy(tracer.at[p], q.at[p], q_sem.at[p]).wait()
            for k in range(levels):
                for depth in range(DEPTH):
                    x = depth * levels + k
                    s[parity, 3, n, x] = q[p, k, depth:depth + 1, :]
                    s[parity, 1, n, x] = q[p, k, ct - 1 - depth:ct - depth, :]
                group = n * levels + k
                turned = pltpu.roll(q[p, k], (group * 4 + DEPTH) % 128, 1)
                gathered = jnp.where(lane_group == group, turned, gathered)
        upright = gathered.T
        for n in range(half):
            for k in range(levels):
                base = (n * levels + k) * 4
                s[parity, 2, n, levels + k] = upright[base:base + 1]
                s[parity, 2, n, k] = upright[base + 1:base + 2]
                s[parity, 0, n, k] = upright[base + 2:base + 3]
                s[parity, 0, n, levels + k] = upright[base + 3:base + 4]
        if parity == 0:
            pl.semaphore_wait(barrier, total - 1)
        on, along = edge_state(me, parity, total, across)
        for e in range(4):
            @pl.when(on[e])
            def _():
                slot = ((parity * 4 + e) * across + along[e]) * half

                def spread(i, carry):
                    x = lax.rem(me + i, pieces)
                    src, dst = s.at[parity, e, :, x], r.at[pl.ds(slot, half)]

                    @pl.when(x != me)
                    def _():
                        remote(src, dst, send1.at[parity, e], r_sem, x).start()

                    @pl.when(x == me)
                    def _():
                        pltpu.make_async_copy(src, dst, r_sem).start()

                    return carry

                lax.fori_loop(0, pieces, spread, 0)
        for e in range(4):
            @pl.when(jnp.logical_not(on[e]))
            def _():
                far = (e + 2) % 4
                remote(s.at[parity, e], h.at[parity, far], send1.at[parity, e],
                       h_sem.at[parity, far], lax.rem(me + steps[e], total)).start()

    pltpu.make_async_copy(s, s_out, out_sem.at[0]).start()

    @pl.when(me < pieces)
    def _():
        pltpu.make_async_copy(r, r, r_sem).wait()
        for parity in range(2):
            for e in range(4):
                for n in range(half):
                    p = 2 * n + parity
                    other, f, turn = table[p, e, 0], table[p, e, 1], table[p, e, 2]
                    base = (lax.rem(other, 2) * 4 + f) * across * half + other // 2
                    for spot in range(across):
                        place = jnp.where(turn == 1, across - 1 - spot, spot)
                        d[((parity * 4 + e) * across + spot) * half + n] = r[base + place * half]
                for spot in range(across):
                    owner = (edge_tile(e, spot, across) + parity * (total // 2 + 1)) % total
                    src = d.at[pl.ds(((parity * 4 + e) * across + spot) * half, half)]
                    dst = h.at[parity, e, :, me]

                    @pl.when(me != owner)
                    def _():
                        remote(src, dst, send2.at[parity, e], h_sem.at[parity, e], owner).start()

                    @pl.when(me == owner)
                    def _():
                        pltpu.make_async_copy(src, dst, h_sem.at[parity, e]).start()

    def drain(ref, sem):
        pltpu.make_async_copy(ref, ref, sem).wait()

    for parity in range(2):
        on, along = edge_state(me, parity, total, across)
        for e in range(4):
            drain(h.at[parity, e], h_sem.at[parity, e])
            base = (parity * 4 + e) * across * half

            @pl.when(jnp.logical_and(on[e], me < pieces))
            def _():
                drain(s.at[parity, e, :, pl.ds(0, pieces - 1)], send1.at[parity, e])
                drain(d.at[pl.ds(base, (across - 1) * half)], send2.at[parity, e])

            @pl.when(jnp.logical_and(on[e], me >= pieces))
            def _():
                drain(s.at[parity, e], send1.at[parity, e])

            @pl.when(jnp.logical_not(on[e]))
            def _():
                drain(s.at[parity, e], send1.at[parity, e])

            @pl.when(jnp.logical_and(jnp.logical_not(on[e]), me < pieces))
            def _():
                drain(d.at[pl.ds(base, across * half)], send2.at[parity, e])

    pltpu.make_async_copy(h, h_out, out_sem.at[1]).start()
    pltpu.make_async_copy(s, s_out, out_sem.at[0]).wait()
    pltpu.make_async_copy(h, h_out, out_sem.at[1]).wait()


def update_kernel(total, across, table, q, east, north, coupling, ghost, own, out, rows, cols):
    _, levels, ct, _ = q.shape
    p = pl.program_id(0)
    parity = lax.rem(p, 2)
    on, _ = edge_state(lax.axis_index("tile"), parity, total, across)
    lane = lax.broadcasted_iota(jnp.int32, (levels, 128), 1)

    def ghosts(e):
        turned = jnp.logical_and(on[e], table[p, e, 2] == 1)
        index = jnp.where(turned, 127 - lane, lane)
        return [jnp.take_along_axis(ghost[0, e, 0, depth], index, axis=1) for depth in range(DEPTH)]

    south, east_rows, north_cols, west = (ghosts(e) for e in range(4))
    below1 = south[0] - own[0, 2, 0, 0]
    below2 = south[1] - own[0, 2, 0, 1]
    above1 = north_cols[0] - own[0, 0, 0, 0]
    above2 = north_cols[1] - own[0, 0, 0, 1]

    @pl.when(p == 0)
    def _():
        rows[...] = jnp.zeros_like(rows)

    rows[pl.ds(0, levels, stride=4), :] = -above1
    rows[pl.ds(1, levels, stride=4), :] = 8.0 * above1 - above2
    rows[pl.ds(2, levels, stride=4), :] = below2 - 8.0 * below1
    rows[pl.ds(3, levels, stride=4), :] = below1
    cols[...] = rows[...].T

    size = 16
    wide = lax.broadcasted_iota(jnp.int32, (size, 128), 1)
    rim = jnp.logical_or(wide < DEPTH, wide >= 128 - DEPTH)
    for start in range(0, ct, size):
        ratios, partials = [], []
        for k in range(levels):
            mid = q[0, k, start:start + size]
            if start == 0:
                ext = jnp.concatenate(
                    [west[1][k:k + 1], west[0][k:k + 1], q[0, k, 0:size + DEPTH]], axis=0)
                near = [ext[o:o + size] for o in (0, 1, 3, 4)]
            elif start + size == ct:
                ext = jnp.concatenate(
                    [q[0, k, start - DEPTH:ct], east_rows[0][k:k + 1], east_rows[1][k:k + 1]], axis=0)
                near = [ext[o:o + size] for o in (0, 1, 3, 4)]
            else:
                near = [q[0, k, start + o:start + o + size] for o in (-2, -1, 1, 2)]
            along_i = 8.0 * (near[2] - near[1]) - (near[3] - near[0])
            along_j = 8.0 * (pltpu.roll(mid, 127, 1) - pltpu.roll(mid, 1, 1)) - (
                pltpu.roll(mid, 126, 1) - pltpu.roll(mid, 2, 1))
            patch = pltpu.roll(cols[start:start + size], (126 - 4 * k) % 128, 1)
            along_j = along_j + jnp.where(rim, patch, 0.0)
            forced = mid - (
                east[0, k, start:start + size].astype(jnp.float32) * along_i
                + north[0, k, start:start + size].astype(jnp.float32) * along_j) * (1.0 / 12.0)
            here = coupling[0, k, start:start + size].astype(jnp.float32)
            if k == 0:
                inverse = 1.0 / (1.0 + here)
                current = forced * inverse
            else:
                inverse = 1.0 / ((1.0 + here) + below * (1.0 - ratios[-1]))
                current = (forced + below * partials[-1]) * inverse
            ratios.append(here * inverse)
            partials.append(current)
            below = here
        value = partials[-1]
        out[0, levels - 1, start:start + size] = value
        for k in range(levels - 2, -1, -1):
            value = partials[k] + ratios[k] * value
            out[0, k, start:start + size] = value


def solution(mesh):
    total = mesh.shape["tile"]
    across = math.isqrt(total)

    def shards(tracer, courant_east, courant_north, diffusivity, seam_table):
        _, panels, levels, ct, _ = tracer.shape
        half, pieces = panels // 2, DEPTH * levels
        strips = (2, 4, half, pieces, 1, ct)
        units = (2 * 4 * across * half, 1, ct)
        anywhere = pl.BlockSpec(memory_space=pl.ANY)
        ghost, own = pl.pallas_call(
            functools.partial(exchange_kernel, total, across),
            out_shape=[jax.ShapeDtypeStruct(strips, jnp.float32)] * 2,
            in_specs=[pl.BlockSpec(memory_space=pltpu.SMEM), anywhere],
            out_specs=[anywhere, anywhere],
            scratch_shapes=[
                pltpu.VMEM(tracer.shape[1:], jnp.float32),
                pltpu.VMEM(strips, jnp.float32),
                pltpu.VMEM(units, jnp.float32),
                pltpu.VMEM(units, jnp.float32),
                pltpu.VMEM(strips, jnp.float32),
                pltpu.SemaphoreType.DMA((panels,)),
                pltpu.SemaphoreType.DMA((2, 4)),
                pltpu.SemaphoreType.DMA,
                pltpu.SemaphoreType.DMA((2, 4)),
                pltpu.SemaphoreType.DMA((2, 4)),
                pltpu.SemaphoreType.DMA((2,)),
            ],
            compiler_params=pltpu.CompilerParams(collective_id=0, has_side_effects=True),
            name="exchange",
        )(seam_table, tracer[0])
        dense = (2, 4, half, DEPTH, levels, ct)
        strip_spec = pl.BlockSpec((1, 4, 1, DEPTH, levels, ct), lambda p: (p % 2, 0, p // 2, 0, 0, 0))
        field = pl.BlockSpec((1, levels, ct, ct), lambda p: (p, 0, 0, 0))
        updated = pl.pallas_call(
            functools.partial(update_kernel, total, across),
            grid=(panels,),
            out_shape=jax.ShapeDtypeStruct(tracer.shape[1:], jnp.float32),
            in_specs=[pl.BlockSpec(memory_space=pltpu.SMEM), field, field, field, field,
                      strip_spec, strip_spec],
            out_specs=field,
            scratch_shapes=[pltpu.VMEM((ct, ct), jnp.float32), pltpu.VMEM((ct, ct), jnp.float32)],
            name="update",
        )(seam_table, tracer[0], courant_east[0], courant_north[0], diffusivity[0],
          ghost.reshape(dense), own.reshape(dense))
        return updated[None]

    placed = P(("groups", "tile"), None, None, None, None)
    return jax.shard_map(
        shards, mesh=mesh, in_specs=(placed, placed, placed, placed, P()), out_specs=placed,
        check_vma=False)
```

```python
import functools
import math

import jax
import jax.numpy as jnp
from jax import lax
from jax.experimental import pallas as pl
from jax.experimental.pallas import tpu as pltpu
from jax.sharding import PartitionSpec as P

DEPTH = 2


def tile_of(device, parity, total):
    return lax.rem(device + total - parity * (total // 2 + 1) + total, total)


def edge_state(device, parity, total, across):
    tile = tile_of(device, parity, total)
    row, col = tile // across, lax.rem(tile, across)
    on = (col == 0, row == across - 1, col == across - 1, row == 0)
    return on, (row, col, row, col)


def edge_tile(edge, spot, across):
    return (spot * across, (across - 1) * across + spot, spot * across + across - 1, spot)[edge]


def central(q, p, k, start, size):
    ct = q.shape[2]
    mid = q[p, k, start:start + size]
    none = jnp.zeros((DEPTH, 128), jnp.float32)
    if start == 0:
        ext = jnp.concatenate([none, q[p, k, 0:size + DEPTH]], axis=0)
        near = [ext[o:o + size] for o in (0, 1, 3, 4)]
    elif start + size == ct:
        ext = jnp.concatenate([q[p, k, start - DEPTH:ct], none], axis=0)
        near = [ext[o:o + size] for o in (0, 1, 3, 4)]
    else:
        near = [q[p, k, start + o:start + o + size] for o in (-2, -1, 1, 2)]
    along_i = 8.0 * (near[2] - near[1]) - (near[3] - near[0])
    along_j = 8.0 * (pltpu.roll(mid, 127, 1) - pltpu.roll(mid, 1, 1)) - (
        pltpu.roll(mid, 126, 1) - pltpu.roll(mid, 2, 1))
    return mid, along_i, along_j


def solve(forced, coupling, levels):
    ratios, partials = [], []
    for k in range(levels):
        value, here = forced(k), coupling(k)
        if k == 0:
            inverse = 1.0 / (1.0 + here)
            current = value * inverse
        else:
            inverse = 1.0 / ((1.0 + here) + below * (1.0 - ratios[-1]))
            current = (value + below * partials[-1]) * inverse
        ratios.append(here * inverse)
        partials.append(current)
        below = here
    solved = [partials[-1]]
    for k in range(levels - 2, -1, -1):
        solved.insert(0, partials[k] + ratios[k] * solved[0])
    return solved


def update_panel(q, east, north, coupling, u, p):
    _, levels, ct, _ = q.shape
    size = 16
    for start in range(0, ct, size):
        part = pl.ds(start, size)

        def forced(k):
            mid, along_i, along_j = central(q, p, k, start, size)
            return mid - (east[p, k, part].astype(jnp.float32) * along_i
                          + north[p, k, part].astype(jnp.float32) * along_j) * (1.0 / 12.0)

        solved = solve(forced, lambda k: coupling[p, k, part].astype(jnp.float32), levels)
        for k in range(levels):
            u[p, k, part] = solved[k]


def rim_columns(field, parity, half, levels, ct):
    lane_group = lax.broadcasted_iota(jnp.int32, (ct, 128), 1) // 4
    gathered = jnp.zeros((ct, 128), jnp.float32)
    for n in range(half):
        for k in range(levels):
            group = n * levels + k
            turned = pltpu.roll(field[2 * n + parity, k].astype(jnp.float32), (group * 4 + DEPTH) % 128, 1)
            gathered = jnp.where(lane_group == group, turned, gathered)
    return gathered.T


def rim_rows(field, parity, half, levels, ct, out, kind):
    for n in range(half):
        for k in range(levels):
            base = (n * levels + k) * 4
            out[kind, parity, base:base + 2] = field[2 * n + parity, k, ct - 16:ct].astype(jnp.float32)[14:16]
            out[kind, parity, base + 2:base + 4] = field[2 * n + parity, k, 0:16].astype(jnp.float32)[0:2]


def exchange_kernel(total, across, table, tracer, east_in, north_in, coupling_in, h_out, rim_out, u_out,
                    q, east, north, coupling, u, rim, s, r, d, h,
                    q_sem, c_sem, send1, r_sem, send2, h_sem, out_sem, u_sem):
    panels, levels, ct, _ = q.shape
    half = panels // 2
    pieces = DEPTH * levels
    me = lax.axis_index("tile")
    steps = (total - 1, across, 1, total - across)

    for p in range(panels):
        pltpu.make_async_copy(tracer.at[p], q.at[p], q_sem.at[p]).start()
    fields = ((east_in, east), (north_in, north), (coupling_in, coupling))
    for i, (src, dst) in enumerate(fields):
        pltpu.make_async_copy(src, dst, c_sem.at[i]).start()

    barrier = pltpu.get_barrier_semaphore()

    def greet(i, carry):
        pl.semaphore_signal(barrier, inc=1, device_id={"tile": lax.rem(me + i, total)},
                            device_id_type=pl.DeviceIdType.MESH)
        return carry

    lax.fori_loop(1, total, greet, 0)

    def remote(src, dst, send, recv, device):
        return pltpu.make_async_remote_copy(
            src_ref=src, dst_ref=dst, send_sem=send, recv_sem=recv,
            device_id={"tile": device}, device_id_type=pl.DeviceIdType.MESH)

    for parity in range(2):
        for n in range(half):
            p = 2 * n + parity
            pltpu.make_async_copy(tracer.at[p], q.at[p], q_sem.at[p]).wait()
            for k in range(levels):
                for depth in range(DEPTH):
                    x = depth * levels + k
                    s[parity, 3, n, x] = q[p, k, depth:depth + 1, :]
                    s[parity, 1, n, x] = q[p, k, ct - 1 - depth:ct - depth, :]
        upright = rim_columns(q, parity, half, levels, ct)
        rim[0, parity] = upright
        for n in range(half):
            for k in range(levels):
                base = (n * levels + k) * 4
                s[parity, 2, n, levels + k] = upright[base:base + 1]
                s[parity, 2, n, k] = upright[base + 1:base + 2]
                s[parity, 0, n, k] = upright[base + 2:base + 3]
                s[parity, 0, n, levels + k] = upright[base + 3:base + 4]
        if parity == 0:
            pl.semaphore_wait(barrier, total - 1)
        on, along = edge_state(me, parity, total, across)
        for e in range(4):
            @pl.when(on[e])
            def _():
                slot = ((parity * 4 + e) * across + along[e]) * half

                def spread(i, carry):
                    x = lax.rem(me + i, pieces)
                    src, dst = s.at[parity, e, :, x], r.at[pl.ds(slot, half)]

                    @pl.when(x != me)
                    def _():
                        remote(src, dst, send1.at[parity, e], r_sem, x).start()

                    @pl.when(x == me)
                    def _():
                        pltpu.make_async_copy(src, dst, r_sem).start()

                    return carry

                lax.fori_loop(0, pieces, spread, 0)
        for e in range(4):
            @pl.when(jnp.logical_not(on[e]))
            def _():
                far = (e + 2) % 4
                remote(s.at[parity, e], h.at[parity, far], send1.at[parity, e],
                       h_sem.at[parity, far], lax.rem(me + steps[e], total)).start()

    def compute(first, last, parity):
        def one(p, carry):
            update_panel(q, east, north, coupling, u, p)
            pltpu.make_async_copy(u.at[p], u_out.at[p], u_sem.at[p]).start()
            return carry

        lax.fori_loop(first, last, one, 0)
        rim[1, parity] = rim_columns(north, parity, half, levels, ct)
        rim[2, parity] = rim_columns(coupling, parity, half, levels, ct)
        rim_rows(east, parity, half, levels, ct, rim, 3)
        rim_rows(coupling, parity, half, levels, ct, rim, 4)

    for i, (src, dst) in enumerate(fields):
        pltpu.make_async_copy(src, dst, c_sem.at[i]).wait()
    compute(0, half, 0)

    @pl.when(me < pieces)
    def _():
        pltpu.make_async_copy(r, r, r_sem).wait()
        for parity in range(2):
            for e in range(4):
                for n in range(half):
                    p = 2 * n + parity
                    other, f, turn = table[0, e, p], table[1, e, p], table[2, e, p]
                    base = (lax.rem(other, 2) * 4 + f) * across * half + other // 2
                    for spot in range(across):
                        place = jnp.where(turn == 1, across - 1 - spot, spot)
                        d[((parity * 4 + e) * across + spot) * half + n] = r[base + place * half]
                for spot in range(across):
                    owner = (edge_tile(e, spot, across) + parity * (total // 2 + 1)) % total
                    src = d.at[pl.ds(((parity * 4 + e) * across + spot) * half, half)]
                    dst = h.at[parity, e, :, me]

                    @pl.when(me != owner)
                    def _():
                        remote(src, dst, send2.at[parity, e], h_sem.at[parity, e], owner).start()

                    @pl.when(me == owner)
                    def _():
                        pltpu.make_async_copy(src, dst, h_sem.at[parity, e]).start()

    compute(half, panels, 1)
    pltpu.make_async_copy(rim, rim_out, out_sem.at[0]).start()

    def drain(ref, sem):
        pltpu.make_async_copy(ref, ref, sem).wait()

    for parity in range(2):
        on, along = edge_state(me, parity, total, across)
        for e in range(4):
            drain(h.at[parity, e], h_sem.at[parity, e])
            base = (parity * 4 + e) * across * half

            @pl.when(jnp.logical_and(on[e], me < pieces))
            def _():
                drain(s.at[parity, e, :, pl.ds(0, pieces - 1)], send1.at[parity, e])
                drain(d.at[pl.ds(base, (across - 1) * half)], send2.at[parity, e])

            @pl.when(jnp.logical_and(on[e], me >= pieces))
            def _():
                drain(s.at[parity, e], send1.at[parity, e])

            @pl.when(jnp.logical_not(on[e]))
            def _():
                drain(s.at[parity, e], send1.at[parity, e])

            @pl.when(jnp.logical_and(jnp.logical_not(on[e]), me < pieces))
            def _():
                drain(d.at[pl.ds(base, across * half)], send2.at[parity, e])

    pltpu.make_async_copy(h, h_out, out_sem.at[1]).start()
    pltpu.make_async_copy(rim, rim_out, out_sem.at[0]).wait()
    pltpu.make_async_copy(h, h_out, out_sem.at[1]).wait()
    for p in range(panels):
        pltpu.make_async_copy(u.at[p], u_out.at[p], u_sem.at[p]).wait()


def correct_kernel(total, across, table, u, ghost, rim, out, change, cols):
    _, levels, ct, _ = u.shape
    half = ghost.shape[2]
    now = pl.program_id(0)

    @pl.when(now == 0)
    def _():
        lane = lax.broadcasted_iota(jnp.int32, (levels, 128), 1)
        for parity in range(2):
            on, _ = edge_state(lax.axis_index("tile"), parity, total, across)
            change[0, parity] = jnp.zeros((ct, 128), jnp.float32)
            for n in range(half):
                p = 2 * n + parity
                base = n * levels * 4

                def ghosts(e):
                    turned = jnp.logical_and(on[e], table[2, e, p] == 1)
                    index = jnp.where(turned, 127 - lane, lane)
                    return [jnp.take_along_axis(ghost[parity, e, n, depth], index, axis=1)
                            for depth in range(DEPTH)]

                south, east, north, west = (ghosts(e) for e in range(4))
                own = [rim[0, parity, pl.ds(base + c, levels, stride=4)] for c in range(4)]
                sides = ((north[0] - own[2], north[1] - own[3], south[0] - own[1], south[1] - own[0]),
                         (east[0], east[1], west[0], west[1]))
                for way, (above1, above2, below1, below2) in enumerate(sides):
                    values = (-above1, 8.0 * above1 - above2, below2 - 8.0 * below1, below1)
                    for c, value in enumerate(values):
                        change[way, parity, pl.ds(base + c, levels, stride=4)] = value
                for way in range(2):
                    def rows(k):
                        return pl.ds(base + 4 * k, 4)

                    solved = solve(
                        lambda k: change[way, parity, rows(k)] * rim[1 + 2 * way, parity, rows(k)] * (-1.0 / 12.0),
                        lambda k: rim[2 + 2 * way, parity, rows(k)], levels)
                    for k in range(levels):
                        change[way, parity, rows(k)] = solved[k]
            cols[parity] = change[0, parity].T

    size = 16
    wide = lax.broadcasted_iota(jnp.int32, (size, 128), 1)
    edge = jnp.logical_or(wide < DEPTH, wide >= 128 - DEPTH)
    for p in range(2 * half):
        @pl.when(now == p)
        def _():
            parity, n = p % 2, p // 2
            for k in range(levels):
                base = (n * levels + k) * 4
                for start in range(0, ct, size):
                    patch = pltpu.roll(cols[parity, start:start + size], (126 - base) % 128, 1)
                    out[0, k, start:start + size] = u[0, k, start:start + size] + jnp.where(edge, patch, 0.0)
                out[0, k, ct - DEPTH:ct] = out[0, k, ct - DEPTH:ct] + change[1, parity, base:base + 2]
                out[0, k, 0:DEPTH] = out[0, k, 0:DEPTH] + change[1, parity, base + 2:base + 4]


def solution(mesh):
    total = mesh.shape["tile"]
    across = math.isqrt(total)

    def shards(tracer, courant_east, courant_north, diffusivity, seam_table):
        _, panels, levels, ct, _ = tracer.shape
        half, pieces = panels // 2, DEPTH * levels
        strips = (2, 4, half, pieces, 1, ct)
        units = (2 * 4 * across * half, 1, ct)
        rims = (5, 2, ct, ct)
        shape = tracer.shape[1:]
        anywhere = pl.BlockSpec(memory_space=pl.ANY)
        scalars = pl.BlockSpec(memory_space=pltpu.SMEM)
        table = jnp.transpose(seam_table, (2, 1, 0))
        ghost, rim, plain = pl.pallas_call(
            functools.partial(exchange_kernel, total, across),
            out_shape=[jax.ShapeDtypeStruct(dims, jnp.float32) for dims in (strips, rims, shape)],
            in_specs=[scalars] + [anywhere] * 4,
            out_specs=[anywhere] * 3,
            scratch_shapes=[
                pltpu.VMEM(shape, jnp.float32),
                pltpu.VMEM(shape, jnp.bfloat16),
                pltpu.VMEM(shape, jnp.bfloat16),
                pltpu.VMEM(shape, jnp.bfloat16),
                pltpu.VMEM(shape, jnp.float32),
                pltpu.VMEM(rims, jnp.float32),
                pltpu.VMEM(strips, jnp.float32),
                pltpu.VMEM(units, jnp.float32),
                pltpu.VMEM(units, jnp.float32),
                pltpu.VMEM(strips, jnp.float32),
                pltpu.SemaphoreType.DMA((panels,)),
                pltpu.SemaphoreType.DMA((3,)),
                pltpu.SemaphoreType.DMA((2, 4)),
                pltpu.SemaphoreType.DMA,
                pltpu.SemaphoreType.DMA((2, 4)),
                pltpu.SemaphoreType.DMA((2, 4)),
                pltpu.SemaphoreType.DMA((2,)),
                pltpu.SemaphoreType.DMA((panels,)),
            ],
            compiler_params=pltpu.CompilerParams(collective_id=0, has_side_effects=True),
            name="exchange",
        )(table, tracer[0], courant_east[0], courant_north[0], diffusivity[0])
        dense = (2, 4, half, DEPTH, levels, ct)
        field = pl.BlockSpec((1, levels, ct, ct), lambda p: (p, 0, 0, 0))
        whole = pl.BlockSpec(memory_space=pltpu.VMEM)
        updated = pl.pallas_call(
            functools.partial(correct_kernel, total, across),
            grid=(panels,),
            out_shape=jax.ShapeDtypeStruct(shape, jnp.float32),
            in_specs=[scalars, field, whole, whole],
            out_specs=field,
            scratch_shapes=[pltpu.VMEM((2, 2, ct, ct), jnp.float32), pltpu.VMEM((2, ct, ct), jnp.float32)],
            name="correct",
        )(table, plain, ghost.reshape(dense), rim)
        return updated[None]

    placed = P(("groups", "tile"), None, None, None, None)
    return jax.shard_map(
        shards, mesh=mesh, in_specs=(placed, placed, placed, placed, P()), out_specs=placed,
        check_vma=False)
```

```python
import functools
import math

import jax
import jax.numpy as jnp
from jax import lax
from jax.experimental import pallas as pl
from jax.experimental.pallas import tpu as pltpu
from jax.sharding import PartitionSpec as P

DEPTH = 2
VMEM_LIMIT = 59 * 1024 * 1024


def tile_of(device, parity, total):
    return lax.rem(device + total - parity * (total // 2 + 1) + total, total)


def edge_state(device, parity, total, across):
    tile = tile_of(device, parity, total)
    row, col = tile // across, lax.rem(tile, across)
    on = (col == 0, row == across - 1, col == across - 1, row == 0)
    return on, (row, col, row, col)


def edge_tile(edge, spot, across):
    return (spot * across, (across - 1) * across + spot, spot * across + across - 1, spot)[edge]


def central(q, p, k, start, size):
    ct = q.shape[2]
    mid = q[p, k, start:start + size]
    none = jnp.zeros((DEPTH, 128), jnp.float32)
    if start == 0:
        ext = jnp.concatenate([none, q[p, k, 0:size + DEPTH]], axis=0)
        near = [ext[o:o + size] for o in (0, 1, 3, 4)]
    elif start + size == ct:
        ext = jnp.concatenate([q[p, k, start - DEPTH:ct], none], axis=0)
        near = [ext[o:o + size] for o in (0, 1, 3, 4)]
    else:
        near = [q[p, k, start + o:start + o + size] for o in (-2, -1, 1, 2)]
    along_i = 8.0 * (near[2] - near[1]) - (near[3] - near[0])
    along_j = 8.0 * (pltpu.roll(mid, 127, 1) - pltpu.roll(mid, 1, 1)) - (
        pltpu.roll(mid, 126, 1) - pltpu.roll(mid, 2, 1))
    return mid, along_i, along_j


def solve(forced, coupling, levels):
    ratios, partials = [], []
    for k in range(levels):
        value, here = forced(k), coupling(k)
        if k == 0:
            inverse = 1.0 / (1.0 + here)
            current = value * inverse
        else:
            inverse = 1.0 / ((1.0 + here) + below * (1.0 - ratios[-1]))
            current = (value + below * partials[-1]) * inverse
        ratios.append(here * inverse)
        partials.append(current)
        below = here
    solved = [partials[-1]]
    for k in range(levels - 2, -1, -1):
        solved.insert(0, partials[k] + ratios[k] * solved[0])
    return solved


def update_panel(q, east, north, coupling, u, p):
    _, levels, ct, _ = q.shape
    size = 16
    for start in range(0, ct, size):
        part = pl.ds(start, size)

        def forced(k):
            mid, along_i, along_j = central(q, p, k, start, size)
            return mid - (east[p, k, part].astype(jnp.float32) * along_i
                          + north[p, k, part].astype(jnp.float32) * along_j) * (1.0 / 12.0)

        solved = solve(forced, lambda k: coupling[p, k, part].astype(jnp.float32), levels)
        for k in range(levels):
            u[p, k, part] = solved[k]


def rim_columns(field, parity, half, levels, ct):
    lane_group = lax.broadcasted_iota(jnp.int32, (ct, 128), 1) // 4
    gathered = jnp.zeros((ct, 128), jnp.float32)
    for n in range(half):
        for k in range(levels):
            group = n * levels + k
            turned = pltpu.roll(field[2 * n + parity, k].astype(jnp.float32), (group * 4 + DEPTH) % 128, 1)
            gathered = jnp.where(lane_group == group, turned, gathered)
    return gathered.T


def rim_rows(field, parity, half, levels, ct, out, kind):
    for n in range(half):
        for k in range(levels):
            base = (n * levels + k) * 4
            out[kind, parity, base:base + 2] = field[2 * n + parity, k, ct - 16:ct].astype(jnp.float32)[14:16]
            out[kind, parity, base + 2:base + 4] = field[2 * n + parity, k, 0:16].astype(jnp.float32)[0:2]


def exchange_kernel(total, across, table, tracer, east_in, north_in, coupling_in, h_out, rim, u,
                    q, east, north, coupling, s, r, d, h,
                    q_sem, c_sem, send1, r_sem, send2, h_sem, out_sem):
    panels, levels, ct, _ = q.shape
    half = panels // 2
    pieces = DEPTH * levels
    me = lax.axis_index("tile")
    steps = (total - 1, across, 1, total - across)

    for p in range(panels):
        pltpu.make_async_copy(tracer.at[p], q.at[p], q_sem.at[p]).start()
    fields = ((east_in, east), (north_in, north), (coupling_in, coupling))
    for i, (src, dst) in enumerate(fields):
        pltpu.make_async_copy(src, dst, c_sem.at[i]).start()

    barrier = pltpu.get_barrier_semaphore()

    def greet(i, carry):
        pl.semaphore_signal(barrier, inc=1, device_id={"tile": lax.rem(me + i, total)},
                            device_id_type=pl.DeviceIdType.MESH)
        return carry

    lax.fori_loop(1, total, greet, 0)

    def remote(src, dst, send, recv, device):
        return pltpu.make_async_remote_copy(
            src_ref=src, dst_ref=dst, send_sem=send, recv_sem=recv,
            device_id={"tile": device}, device_id_type=pl.DeviceIdType.MESH)

    for parity in range(2):
        for n in range(half):
            p = 2 * n + parity
            pltpu.make_async_copy(tracer.at[p], q.at[p], q_sem.at[p]).wait()
            for k in range(levels):
                for depth in range(DEPTH):
                    x = depth * levels + k
                    s[parity, 3, n, x] = q[p, k, depth:depth + 1, :]
                    s[parity, 1, n, x] = q[p, k, ct - 1 - depth:ct - depth, :]
        upright = rim_columns(q, parity, half, levels, ct)
        rim[0, parity] = upright
        for n in range(half):
            for k in range(levels):
                base = (n * levels + k) * 4
                s[parity, 2, n, levels + k] = upright[base:base + 1]
                s[parity, 2, n, k] = upright[base + 1:base + 2]
                s[parity, 0, n, k] = upright[base + 2:base + 3]
                s[parity, 0, n, levels + k] = upright[base + 3:base + 4]
        if parity == 0:
            pl.semaphore_wait(barrier, total - 1)
        on, along = edge_state(me, parity, total, across)
        for e in range(4):
            @pl.when(on[e])
            def _():
                slot = ((parity * 4 + e) * across + along[e]) * half

                def spread(i, carry):
                    x = lax.rem(me + i, pieces)
                    src, dst = s.at[parity, e, :, x], r.at[pl.ds(slot, half)]

                    @pl.when(x != me)
                    def _():
                        remote(src, dst, send1.at[parity, e], r_sem, x).start()

                    @pl.when(x == me)
                    def _():
                        pltpu.make_async_copy(src, dst, r_sem).start()

                    return carry

                lax.fori_loop(0, pieces, spread, 0)
        for e in range(4):
            @pl.when(jnp.logical_not(on[e]))
            def _():
                far = (e + 2) % 4
                remote(s.at[parity, e], h.at[parity, far], send1.at[parity, e],
                       h_sem.at[parity, far], lax.rem(me + steps[e], total)).start()

    def compute(first, last, parity):
        def one(p, carry):
            update_panel(q, east, north, coupling, u, p)
            return carry

        lax.fori_loop(first, last, one, 0)
        rim[1, parity] = rim_columns(north, parity, half, levels, ct)
        rim[2, parity] = rim_columns(coupling, parity, half, levels, ct)
        rim_rows(east, parity, half, levels, ct, rim, 3)
        rim_rows(coupling, parity, half, levels, ct, rim, 4)

    for i, (src, dst) in enumerate(fields):
        pltpu.make_async_copy(src, dst, c_sem.at[i]).wait()
    compute(0, half, 0)

    @pl.when(me < pieces)
    def _():
        pltpu.make_async_copy(r, r, r_sem).wait()
        for parity in range(2):
            for e in range(4):
                for n in range(half):
                    p = 2 * n + parity
                    other, f, turn = table[0, e, p], table[1, e, p], table[2, e, p]
                    base = (lax.rem(other, 2) * 4 + f) * across * half + other // 2
                    for spot in range(across):
                        place = jnp.where(turn == 1, across - 1 - spot, spot)
                        d[((parity * 4 + e) * across + spot) * half + n] = r[base + place * half]
                for spot in range(across):
                    owner = (edge_tile(e, spot, across) + parity * (total // 2 + 1)) % total
                    src = d.at[pl.ds(((parity * 4 + e) * across + spot) * half, half)]
                    dst = h.at[parity, e, :, me]

                    @pl.when(me != owner)
                    def _():
                        remote(src, dst, send2.at[parity, e], h_sem.at[parity, e], owner).start()

                    @pl.when(me == owner)
                    def _():
                        pltpu.make_async_copy(src, dst, h_sem.at[parity, e]).start()

    compute(half, panels, 1)

    def drain(ref, sem):
        pltpu.make_async_copy(ref, ref, sem).wait()

    for parity in range(2):
        on, along = edge_state(me, parity, total, across)
        for e in range(4):
            drain(h.at[parity, e], h_sem.at[parity, e])
            base = (parity * 4 + e) * across * half

            @pl.when(jnp.logical_and(on[e], me < pieces))
            def _():
                drain(s.at[parity, e, :, pl.ds(0, pieces - 1)], send1.at[parity, e])
                drain(d.at[pl.ds(base, (across - 1) * half)], send2.at[parity, e])

            @pl.when(jnp.logical_and(on[e], me >= pieces))
            def _():
                drain(s.at[parity, e], send1.at[parity, e])

            @pl.when(jnp.logical_not(on[e]))
            def _():
                drain(s.at[parity, e], send1.at[parity, e])

            @pl.when(jnp.logical_and(jnp.logical_not(on[e]), me < pieces))
            def _():
                drain(d.at[pl.ds(base, across * half)], send2.at[parity, e])

    pltpu.make_async_copy(h, h_out, out_sem).start()
    pltpu.make_async_copy(h, h_out, out_sem).wait()


def correct_kernel(total, across, table, u, ghost, rim, result, change, cols, out, out_sem):
    _, levels, ct, _ = u.shape
    half = ghost.shape[2]
    lane = lax.broadcasted_iota(jnp.int32, (levels, 128), 1)
    size = 16
    wide = lax.broadcasted_iota(jnp.int32, (size, 128), 1)
    edge = jnp.logical_or(wide < DEPTH, wide >= 128 - DEPTH)
    for parity in range(2):
        on, _ = edge_state(lax.axis_index("tile"), parity, total, across)
        change[0, parity] = jnp.zeros((ct, 128), jnp.float32)
        for n in range(half):
            p = 2 * n + parity
            base = n * levels * 4

            def ghosts(e):
                turned = jnp.logical_and(on[e], table[2, e, p] == 1)
                index = jnp.where(turned, 127 - lane, lane)
                return [jnp.take_along_axis(ghost[parity, e, n, depth], index, axis=1)
                        for depth in range(DEPTH)]

            south, east, north, west = (ghosts(e) for e in range(4))
            own = [rim[0, parity, pl.ds(base + c, levels, stride=4)] for c in range(4)]
            sides = ((north[0] - own[2], north[1] - own[3], south[0] - own[1], south[1] - own[0]),
                     (east[0], east[1], west[0], west[1]))
            for way, (above1, above2, below1, below2) in enumerate(sides):
                values = (-above1, 8.0 * above1 - above2, below2 - 8.0 * below1, below1)
                for c, value in enumerate(values):
                    change[way, parity, pl.ds(base + c, levels, stride=4)] = value
            for way in range(2):
                def rows(k):
                    return pl.ds(base + 4 * k, 4)

                solved = solve(
                    lambda k: change[way, parity, rows(k)] * rim[1 + 2 * way, parity, rows(k)] * (-1.0 / 12.0),
                    lambda k: rim[2 + 2 * way, parity, rows(k)], levels)
                for k in range(levels):
                    change[way, parity, rows(k)] = solved[k]
        cols[parity] = change[0, parity].T

        for n in range(half):
            p = 2 * n + parity
            for k in range(levels):
                base = (n * levels + k) * 4
                for start in range(0, ct, size):
                    patch = pltpu.roll(cols[parity, start:start + size], (126 - base) % 128, 1)
                    out[p, k, start:start + size] = u[p, k, start:start + size] + jnp.where(edge, patch, 0.0)
                out[p, k, ct - DEPTH:ct] = out[p, k, ct - DEPTH:ct] + change[1, parity, base:base + 2]
                out[p, k, 0:DEPTH] = out[p, k, 0:DEPTH] + change[1, parity, base + 2:base + 4]
            pltpu.make_async_copy(out.at[p], result.at[p], out_sem.at[p]).start()
    for p in range(2 * half):
        pltpu.make_async_copy(out.at[p], result.at[p], out_sem.at[p]).wait()


def solution(mesh):
    total = mesh.shape["tile"]
    across = math.isqrt(total)

    def shards(tracer, courant_east, courant_north, diffusivity, seam_table):
        _, panels, levels, ct, _ = tracer.shape
        half, pieces = panels // 2, DEPTH * levels
        strips = (2, 4, half, pieces, 1, ct)
        units = (2 * 4 * across * half, 1, ct)
        rims = (5, 2, ct, ct)
        shape = tracer.shape[1:]
        anywhere = pl.BlockSpec(memory_space=pl.ANY)
        whole = pl.BlockSpec(memory_space=pltpu.VMEM)
        scalars = pl.BlockSpec(memory_space=pltpu.SMEM)
        table = jnp.transpose(seam_table, (2, 1, 0))
        ghost, rim, plain = pl.pallas_call(
            functools.partial(exchange_kernel, total, across),
            out_shape=[pltpu.VMEM(dims, jnp.float32) for dims in (strips, rims, shape)],
            in_specs=[scalars] + [pl.BlockSpec(memory_space=pltpu.HBM)] * 4,
            out_specs=[whole] * 3,
            scratch_shapes=[
                pltpu.VMEM(shape, jnp.float32),
                pltpu.VMEM(shape, jnp.bfloat16),
                pltpu.VMEM(shape, jnp.bfloat16),
                pltpu.VMEM(shape, jnp.bfloat16),
                pltpu.VMEM(strips, jnp.float32),
                pltpu.VMEM(units, jnp.float32),
                pltpu.VMEM(units, jnp.float32),
                pltpu.VMEM(strips, jnp.float32),
                pltpu.SemaphoreType.DMA((panels,)),
                pltpu.SemaphoreType.DMA((3,)),
                pltpu.SemaphoreType.DMA((2, 4)),
                pltpu.SemaphoreType.DMA,
                pltpu.SemaphoreType.DMA((2, 4)),
                pltpu.SemaphoreType.DMA((2, 4)),
                pltpu.SemaphoreType.DMA,
            ],
            compiler_params=pltpu.CompilerParams(collective_id=0, has_side_effects=True,
                                                 vmem_limit_bytes=VMEM_LIMIT),
            name="exchange",
        )(table, tracer[0], courant_east[0], courant_north[0], diffusivity[0])
        dense = (2, 4, half, DEPTH, levels, ct)
        updated = pl.pallas_call(
            functools.partial(correct_kernel, total, across),
            out_shape=jax.ShapeDtypeStruct(shape, jnp.float32),
            in_specs=[scalars, whole, whole, whole],
            out_specs=anywhere,
            scratch_shapes=[pltpu.VMEM((2, 2, ct, ct), jnp.float32), pltpu.VMEM((2, ct, ct), jnp.float32),
                            pltpu.VMEM(shape, jnp.float32), pltpu.SemaphoreType.DMA((panels,))],
            compiler_params=pltpu.CompilerParams(vmem_limit_bytes=VMEM_LIMIT // 2),
            name="correct",
        )(table, plain, ghost.reshape(dense), rim)
        return updated[None]

    placed = P(("groups", "tile"), None, None, None, None)
    return jax.shard_map(
        shards, mesh=mesh, in_specs=(placed, placed, placed, placed, P()), out_specs=placed,
        check_vma=False)
```
